128 devices in a mesh: src: 16 (over y, z), reg: 8 (over x, core).
Axes of the slice: x: 4, y: 4, z: 4, core: 2. Of those that a mesh axis runs over, the one named last changes fastest.
Arguments:
- tiles: bfloat16 [65536, 128, 128], P(('src', 'reg')), may hold values from -0.1875 to 0.1875
- rays: float32 [8192, 128], P(('src', 'reg')), may hold values from -6 to 6
- tile_rows: int32 [65536], P(('src', 'reg')), may hold values from 0 to 63, as said below
- tile_slots: int32 [65536], P(('src', 'reg')), may hold values from 0 to 255, as said below
- tile_count: int32 [128], P(('src', 'reg')), may hold values from 256 to 512, as said below
- wanted: int32 [128, 128, 2], P(('src', 'reg')), may hold values from 0 to 255
Outputs:
- solution: float32 [32768, 128], P(('src', 'reg'))
- right_vector: float32 [32768, 128], P(('src', 'reg'))
The draws below stay inside these ranges and needn't reach their ends.
Inputs may be any that keep to these rules, and one draw needn't show every extreme that they name: `tile_rows`: non-decreasing along each device's 512 tiles. `tile_slots`: the first 256 tiles of each device name every slot once. `tile_count`: some device has all 512 tiles live.
All inputs are finite; a program needn't handle non-finite values.
Results may differ from the reference program's by a relative error of at most 0.024.
Values may be sent and summed in bfloat16 or wider, within the bound.
No kernel may reach another device: no remote copies, remote signals or barrier semaphores. Data moves between devices by JAX's collectives and lax.ppermute only.
A program may use at most 128 MiB of HBM per device.

```python
import jax
import jax.numpy as jnp
from jax import lax

TILE = 128
BLK_DEV = 256
RB_DEV = 64
TILE_SLOTS_EACH = 512
CAP = 2
ITERS = 3
NRAYBLK = 8192
NTILE = 65536
CELL_BLOCK_SLOTS = 256
DEVICES = 128


def draw_tile_rows(key, part):
    device_list = NTILE // TILE_SLOTS_EACH
    values = jax.random.randint(key, (device_list, TILE_SLOTS_EACH), 0, RB_DEV)
    return jnp.sort(values, axis=1).reshape(-1).astype(jnp.int32)


def draw_tile_slots(key, part):
    device_list = NTILE // TILE_SLOTS_EACH
    leading_part, trailing_part = jax.random.split(jax.random.fold_in(key, 7))
    random_keys = jax.random.split(leading_part, device_list)
    running_offsets = jax.vmap(lambda iteration_index: jax.random.permutation(iteration_index, CELL_BLOCK_SLOTS))(random_keys).astype(jnp.int32)
    remaining_part = jax.random.randint(trailing_part, (device_list, TILE_SLOTS_EACH - CELL_BLOCK_SLOTS), 0, CELL_BLOCK_SLOTS).astype(jnp.int32)
    return jnp.concatenate([running_offsets, remaining_part], axis=1).reshape(-1).astype(jnp.int32)


def draw_tile_count(key, part):
    leading_part, trailing_part = jax.random.split(key)
    device_list = NTILE // TILE_SLOTS_EACH
    entry_counts = jax.random.randint(leading_part, (device_list,), CELL_BLOCK_SLOTS, TILE_SLOTS_EACH + 1)
    filled = jax.random.randint(trailing_part, (), 0, device_list)
    return entry_counts.at[filled].set(TILE_SLOTS_EACH).astype(jnp.int32)


def touch_ends(entries, stream_key, low, top_value):
    spot = [jax.random.randint(jax.random.fold_in(stream_key, axis), (), 0, length) for axis, length in enumerate(entries.shape)]
    widest = entries.shape.index(max(entries.shape))
    beside = spot[:widest] + [(spot[widest] + 1) % entries.shape[widest]] + spot[widest + 1:]
    return entries.at[tuple(spot)].set(low).at[tuple(beside)].set(top_value)


def steps_of(stream_key, extent, pieces, smallest, high):
    gain = 1.0
    for position, shards_of in pieces:
        draws = jax.random.uniform(jax.random.fold_in(jax.random.fold_in(stream_key, 6), position), (shards_of,), jnp.float32, smallest / len(pieces), high / len(pieces))
        gain = gain * jnp.repeat(jnp.exp(draws), extent[position] // shards_of).reshape((-1,) + (1,) * (len(extent) - 1 - position))
    return gain


def scatter_about(own_key, extent, spread, limit, pieces=(), kind=jnp.bfloat16):
    values = spread * jax.random.normal(own_key, extent, jnp.float32)
    if pieces:
        values = values * steps_of(own_key, extent, pieces, -0.22, 0.18)
    return jnp.clip(values, -limit, limit).astype(kind)


def setup_inputs(seed: int = 0) -> dict:
    arg_keys = jax.random.split(jax.random.key(seed), 7)
    tiles = scatter_about(arg_keys[0], (NTILE, TILE, TILE), (TILE_SLOTS_EACH * TILE // RB_DEV) ** -0.5, 0.1875, ((0, 128),))
    rays = scatter_about(arg_keys[1], (NRAYBLK, TILE), 1.0, 6.0, ((0, 128),), jnp.float32)
    tile_rows = draw_tile_rows(jax.random.fold_in(arg_keys[6], 71), 0)
    tile_slots = draw_tile_slots(jax.random.fold_in(arg_keys[6], 71), 0)
    tile_count = draw_tile_count(jax.random.fold_in(arg_keys[6], 71), 0)
    wanted = touch_ends(jax.random.randint(arg_keys[5], (DEVICES, DEVICES, CAP), 0, BLK_DEV), jax.random.fold_in(arg_keys[5], 1), 0, BLK_DEV - 1).astype(jnp.int32)
    return {"tiles": tiles, "rays": rays, "tile_rows": tile_rows, "tile_slots": tile_slots, "tile_count": tile_count, "wanted": wanted}


damping = 0.5

def column_blocks(tile_slots, wanted, blocks_dev):
    device_list = wanted.shape[0]
    cap = wanted.shape[2]
    slots = tile_slots.reshape(device_list, -1)
    owner = slots // cap
    within = slots % cap
    asking = jnp.arange(device_list, dtype=jnp.int32)[:, None]
    local = wanted[owner, asking, within]
    return (owner * blocks_dev + local).astype(jnp.int32)

def forward(tiles4, vec_bf, columns, rows, live, row_blocks):

    def one(args):
        tile_set, cols, row_ids, mask = args
        picked = vec_bf[cols].astype(jnp.float32)
        prod = jnp.einsum('tij,tj->ti', tile_set.astype(jnp.float32), picked, precision=lax.Precision.HIGHEST)
        prod = prod * mask[:, None]
        return jax.ops.segment_sum(prod, row_ids, num_segments=row_blocks)
    result = lax.map(one, (tiles4, columns, rows, live))
    return result.reshape(-1, tiles4.shape[-1])

def adjoint(tiles4, ray_bf, columns, rows, live, total_blocks):
    device_list = tiles4.shape[0]
    width = tiles4.shape[-1]
    ray_dev = ray_bf.reshape(device_list, -1, width)

    def step(total, args):
        tile_set, cols, row_ids, mask, ray_set = args
        picked = ray_set[row_ids].astype(jnp.float32)
        contrib = jnp.einsum('tij,ti->tj', tile_set.astype(jnp.float32), picked, precision=lax.Precision.HIGHEST)
        contrib = contrib * mask[:, None]
        return (total.at[cols].add(contrib), None)
    start = jnp.zeros((total_blocks, width), jnp.float32)
    total, _ = lax.scan(step, start, (tiles4, columns, rows, live, ray_dev))
    return total

def reference(tiles, rays, tile_rows, tile_slots, tile_count, wanted):
    device_list = wanted.shape[0]
    width = tiles.shape[-1]
    total_blocks = BLK_DEV * device_list
    tiles4 = tiles.reshape(device_list, -1, width, width)
    per_dev = tiles4.shape[1]
    rows = tile_rows.reshape(device_list, per_dev)
    row_blocks = rays.shape[0] // device_list
    live = (jnp.arange(per_dev, dtype=jnp.int32)[None, :] < tile_count[:, None]).astype(jnp.float32)
    columns = column_blocks(tile_slots, wanted, BLK_DEV)
    u = jnp.zeros_like(rays)
    v = jnp.zeros((total_blocks, width), jnp.float32)
    solution = jnp.zeros((total_blocks, width), jnp.float32)
    w = jnp.zeros((total_blocks, width), jnp.float32)
    uraw = rays
    vraw = v
    alpha = jnp.float32(1.0)
    phibar = jnp.float32(0.0)
    rhobar = jnp.float32(0.0)
    for step in range(ITERS + 1):
        if step > 0:
            uraw = forward(tiles4, vraw.astype(jnp.bfloat16), columns, rows, live, row_blocks) / alpha - alpha * u
        beta = jnp.sqrt(jnp.sum(uraw * uraw))
        u = uraw / beta
        grad = adjoint(tiles4, uraw.astype(jnp.bfloat16), columns, rows, live, total_blocks)
        vraw = grad / beta - beta * v
        alpha_new = jnp.sqrt(jnp.sum(vraw * vraw))
        v_new = vraw / alpha_new
        if step == 0:
            w = v_new
            phibar = beta
            rhobar = alpha_new
        else:
            rhobar1 = jnp.sqrt(rhobar * rhobar + damping * damping)
            phibar = rhobar / rhobar1 * phibar
            rho = jnp.sqrt(rhobar1 * rhobar1 + beta * beta)
            cosine = rhobar1 / rho
            sine = beta / rho
            theta = sine * alpha_new
            rhobar = -cosine * alpha_new
            phi = cosine * phibar
            phibar = sine * phibar
            solution = solution + phi / rho * w
            w = v_new - theta / rho * w
        v = v_new
        alpha = alpha_new
    scale = jnp.sqrt(jnp.float32(total_blocks * width))
    return (solution, v * scale)
```

```python
import functools

import jax
import jax.numpy as jnp
from jax import lax
from jax.experimental import pallas as pl
from jax.experimental.pallas import tpu as pltpu
from jax.sharding import Mesh
from jax.sharding import PartitionSpec as P

BLK_DEV = 256
ITERS = 3
AXES = ("src_0", "src_1", "reg_0", "reg_1")
damping = 0.5

F32 = jnp.float32
BF16 = jnp.bfloat16
ROWS = 4
UNROLL = 64


def iota(shape, axis):
    return lax.broadcasted_iota(jnp.int32, shape, axis)


def dot(a, b, dims=((1,), (0,))):
    return lax.dot_general(a, b, (dims, ((), ())), preferred_element_type=F32)


def two_pieces(x):
    hi = x.astype(BF16)
    lo = (x - hi.astype(F32)).astype(BF16)
    return jnp.concatenate([hi, lo], axis=1)


def exact_dot(onehot, x):
    width = x.shape[1]
    both = dot(onehot, two_pieces(x))
    return both[:, :width] + both[:, width:]


def scalar_row(x, rows, width):
    a = x.astype(BF16).astype(F32)
    b = (x - a).astype(BF16).astype(F32)
    c = x - a - b
    lane = iota((rows, width), 1)
    row = iota((rows, width), 0) & (ROWS - 1)
    v = jnp.where(lane == 0, a, jnp.where(lane == 1, b, jnp.where(lane == 2, c, 0.0)))
    return jnp.where(row == 2, v, 0.0)


def scalar_total(recv):
    rows, width = recv.shape
    lane = iota((rows, width), 1)
    row = iota((rows, width), 0) & (ROWS - 1)
    return total(jnp.where((row == 2) & (lane < 3), recv.astype(F32), 0.0))


def total(x):
    return jnp.sum(jnp.sum(x, axis=0, keepdims=True), axis=1, keepdims=True)


def products(picked_ref, tiles_ref, out_ref, first, transposed):
    row = iota((16, 128), 0)
    if transposed:
        left = ((row & 3) < 2).astype(BF16)
    else:
        left = ((row & 1) == 0).astype(BF16)
    right = 1 - left
    row8 = iota((8, 128), 0)
    low = row8 < 4
    if transposed:
        side = (row8 & 1) == 0
    else:
        side = (row8 & 3) < 2
    dims = ((1,), (1,)) if transposed else ((1,), (0,))
    for pack in range(UNROLL // 16):
        base = first + 16 * pack
        pk = picked_ref[pl.ds(base, 16), :]
        lhs = jnp.concatenate([pk * left, pk * right], axis=1)
        res = []
        for g in range(4):
            wa = tiles_ref[pl.ds(base + 4 * g, 2)].reshape(256, 128)
            wb = tiles_ref[pl.ds(base + 4 * g + 2, 2)].reshape(256, 128)
            res.append(dot(lhs, jnp.concatenate([wa, wb], axis=1), dims))
        for h in range(2):
            a = res[2 * h][8 * h : 8 * h + 8]
            b = res[2 * h + 1][8 * h : 8 * h + 8]
            a = jnp.where(side, a[:, :128], a[:, 128:])
            b = jnp.where(side, b[:, :128], b[:, 128:])
            out_ref[pl.ds(base + 8 * h, 8), :] = jnp.where(low, a, b)


def first_kernel(
    count_ref, tiles_ref, rays_ref, rows_ref, slots_ref, req_ref,
    tiles_out, send_ref, s_ref, st_ref, r_ref, rt_ref, g_ref, gt_ref,
    picked, res, sem,
):
    ntile = tiles_ref.shape[0]
    nrow = rays_ref.shape[0]
    steps = ntile // UNROLL

    def copy(i):
        part = pl.ds(i * UNROLL, UNROLL)
        return pltpu.make_async_copy(tiles_ref.at[part], tiles_out.at[part], sem.at[i])

    for i in range(steps):
        copy(i).start()
    live = iota((1, ntile), 1) < count_ref[0]
    rows = jnp.where(live, rows_ref[...], -1)
    slots = slots_ref[...]
    slots = jnp.where(live, (slots >> 1) * ROWS + (slots & 1), -1)
    rt = (jnp.broadcast_to(rows, (nrow, ntile)) == iota((nrow, ntile), 0)).astype(F32)
    rt_ref[...] = rt.astype(BF16)
    rb = jnp.broadcast_to(rows.astype(F32), (128, ntile)).T.astype(jnp.int32)
    r_ref[...] = (rb == iota((ntile, 128), 1)).astype(F32).astype(BF16)
    nq = st_ref.shape[0]
    for q in range(0, nq, 128):
        st = jnp.broadcast_to(slots, (128, ntile)) == iota((128, ntile), 0) + q
        st_ref[q : q + 128, :] = st.astype(F32).astype(BF16)
    sb = jnp.broadcast_to(slots.astype(F32), (128, ntile)).T.astype(jnp.int32)
    for q in range(0, nq, 128):
        s = sb == iota((ntile, 128), 1) + q
        s_ref[:, q : q + 128] = s.astype(F32).astype(BF16)
    req = req_ref[...]
    gt = jnp.broadcast_to(req, (BLK_DEV, nq)) == iota((BLK_DEV, nq), 0)
    gt_ref[...] = gt.astype(F32).astype(BF16)
    gb = jnp.broadcast_to(req.astype(F32), (128, nq)).T.astype(jnp.int32)
    for q in range(0, BLK_DEV, 128):
        g = gb == iota((nq, 128), 1) + q
        g_ref[:, q : q + 128] = g.astype(F32).astype(BF16)

    uraw = rays_ref[...]
    ub = jnp.concatenate([uraw, jnp.zeros((128 - nrow, 128), F32)], axis=0).astype(BF16)
    picked[...] = dot(r_ref[...], ub).astype(BF16)
    uu = total(uraw * uraw)

    def body(i, carry):
        copy(i).wait()
        products(picked, tiles_out, res, i * UNROLL, False)
        return carry

    lax.fori_loop(0, steps, body, 0)
    sums = exact_dot(st_ref[...], res[...])
    send_ref[...] = (sums + scalar_row(uu, nq, 128)).astype(BF16)


def ray_kernel(
    tiles_ref, recv_ref, s_ref, st_ref, r_ref, rt_ref, uraw_ref, beta_ref,
    send_ref, uraw_out, alpha_ref,
    picked, res,
):
    ntile = tiles_ref.shape[0]
    nrow = uraw_ref.shape[0]
    nq = recv_ref.shape[0]
    steps = ntile // UNROLL
    recv = recv_ref[...]
    alpha = jnp.sqrt(scalar_total(recv))
    picked[...] = dot(s_ref[...], recv).astype(BF16)

    def forward(i, carry):
        products(picked, tiles_ref, res, i * UNROLL, True)
        return carry

    lax.fori_loop(0, steps, forward, 0)
    product = exact_dot(rt_ref[...], res[...])
    beta = beta_ref[0:1, 0:1]
    uraw = product / alpha - alpha * (uraw_ref[...] / beta)
    uraw_out[...] = uraw
    alpha_ref[...] = jnp.broadcast_to(alpha, (8, 128))
    ub = jnp.concatenate([uraw, jnp.zeros((128 - nrow, 128), F32)], axis=0).astype(BF16)
    picked[...] = dot(r_ref[...], ub).astype(BF16)
    uu = total(uraw * uraw)

    def adjoint(i, carry):
        products(picked, tiles_ref, res, i * UNROLL, False)
        return carry

    lax.fori_loop(0, steps, adjoint, 0)
    sums = exact_dot(st_ref[...], res[...])
    send_ref[...] = (sums + scalar_row(uu, nq, 128)).astype(BF16)


def cell_kernel(step, last, *refs):
    recv_ref, gt_ref, g_ref = refs[:3]
    recv = recv_ref[...]
    nq = recv.shape[0]
    beta = jnp.sqrt(scalar_total(recv))
    grad = dot(gt_ref[...], recv)
    if step == 0:
        send_ref, vraw_out, state_out = refs[3:]
        vraw = grad / beta
        zero = jnp.zeros_like(beta)
        state = [beta, beta, zero, zero, zero, zero]
    else:
        if step == 1:
            vraw_ref, alpha_ref, state_ref = refs[3:6]
            w_ref = solution_ref = None
            outs = refs[6:]
        elif step == 2:
            vraw_ref, alpha_ref, state_ref, w_ref, solution_ref = refs[3:8]
            outs = refs[8:]
        else:
            vraw_ref, alpha_ref, state_ref, w_ref, solution_ref = refs[3:8]
            outs = refs[8:]
        alpha = alpha_ref[0:1, 0:1]
        old = [state_ref[i : i + 1, 0:1] for i in range(6)]
        _, phibar, rhobar, cosine, sine, rho = old
        v = vraw_ref[...] / alpha
        vraw = grad / beta - beta * v
        if step == 1:
            w = v
            rhobar = alpha
        else:
            w = v - (sine * alpha / rho) * w_ref[...]
            rhobar = -cosine * alpha
        rhobar1 = jnp.sqrt(rhobar * rhobar + damping * damping)
        phibar = rhobar / rhobar1 * phibar
        rho = jnp.sqrt(rhobar1 * rhobar1 + beta * beta)
        cosine = rhobar1 / rho
        sine = beta / rho
        phi = cosine * phibar
        phibar = sine * phibar
        update = (phi / rho) * w
        solution = update if step == 1 else solution_ref[...] + update
        if last:
            send_ref, vraw_out, solution_out = outs
            solution_out[...] = solution
        else:
            send_ref, vraw_out, state_out, w_out, solution_out = outs
            solution_out[...] = solution
            w_out[...] = w
            state = [beta, phibar, rhobar, cosine, sine, rho]
    vraw_out[...] = vraw
    vv = total(vraw * vraw)
    if last:
        send_ref[...] = jnp.broadcast_to(vv, send_ref.shape)
    else:
        sent = dot(g_ref[...], vraw.astype(BF16))
        send_ref[...] = (sent + scalar_row(vv, nq, 128)).astype(BF16)
        for i, x in enumerate(state):
            state_out[i : i + 1, :] = jnp.broadcast_to(x, (1, 128))


def norm_kernel(scale, recv_ref, vraw_ref, out_ref):
    recv = recv_ref[...]
    vv = jnp.sum(jnp.sum(recv, axis=0, keepdims=True)[:, 0:1], axis=1, keepdims=True)
    out_ref[...] = vraw_ref[...] * (scale / jnp.sqrt(vv))


def shape(dims, dtype=F32):
    return jax.ShapeDtypeStruct(dims, dtype)


def vmem(dims, dtype):
    return pltpu.VMEM(dims, dtype)


def call(kernel, outs, n_in, scratch=(), limit=24 << 20, flops=0, smem=0, hbm=None):
    in_specs = []
    for i in range(n_in):
        if i < smem:
            in_specs.append(pl.BlockSpec(memory_space=pltpu.SMEM))
        elif i == hbm:
            in_specs.append(pl.BlockSpec(memory_space=pl.ANY))
        else:
            in_specs.append(pl.BlockSpec(memory_space=pltpu.VMEM))
    return pl.pallas_call(
        kernel,
        out_shape=outs,
        in_specs=in_specs,
        out_specs=[pl.BlockSpec(memory_space=pltpu.VMEM)] * len(outs),
        scratch_shapes=list(scratch),
        compiler_params=pltpu.CompilerParams(vmem_limit_bytes=limit),
    )


def per_device(tiles, rays, tile_rows, tile_slots, tile_count, wanted):
    ndev = lax.axis_size(AXES)
    ntile, _, width = tiles.shape
    nrow = rays.shape[0]
    cap = wanted.shape[2]
    nq = ndev * ROWS
    req = jnp.concatenate(
        [wanted[0], jnp.full((ndev, ROWS - cap), -1, jnp.int32)], axis=1
    ).reshape(1, nq)

    def exchange(x):
        rows = x.shape[0] // ndev
        y = lax.all_to_all(
            x.reshape(ndev, rows, width), AXES, split_axis=0, concat_axis=0, tiled=True
        )
        return y.reshape(x.shape)

    scratch = [pltpu.VMEM((ntile, width), BF16), pltpu.VMEM((ntile, width), F32)]
    tiles_v, send, s, st, r, rt, g, gt = call(
        first_kernel,
        [
            vmem((ntile, width, width), BF16),
            shape((nq, width), BF16),
            shape((ntile, nq), BF16),
            shape((nq, ntile), BF16),
            shape((ntile, 128), BF16),
            shape((nrow, ntile), BF16),
            shape((nq, BLK_DEV), BF16),
            shape((BLK_DEV, nq), BF16),
        ],
        6,
        scratch + [pltpu.SemaphoreType.DMA((ntile // UNROLL,))],
        smem=1,
        hbm=1,
    )(tile_count, tiles, rays, tile_rows.reshape(1, ntile), tile_slots.reshape(1, ntile), req)

    cells = shape((BLK_DEV, width))
    state_shape = shape((8, width))
    sent = shape((nq, width), BF16)
    uraw = rays
    w = solution = alpha = state = vraw = None
    for step in range(ITERS + 1):
        last = step == ITERS
        if step > 0:
            recv = exchange(send)
            send, uraw, alpha = call(
                ray_kernel,
                [sent, shape((nrow, width)), state_shape],
                8,
                scratch,
            )(pltpu.with_memory_space_constraint(tiles_v, pltpu.VMEM), recv, s, st, r, rt, uraw, state)
        recv = exchange(send)
        if step == 0:
            send, vraw, state = call(
                functools.partial(cell_kernel, step, False), [sent, cells, state_shape], 3
            )(recv, gt, g)
        elif last:
            send, vraw, solution = call(
                functools.partial(cell_kernel, step, True),
                [shape((ndev, width)), cells, cells],
                8,
            )(recv, gt, g, vraw, alpha, state, w, solution)
        else:
            extra = [] if step == 1 else [w, solution]
            send, vraw, state, w, solution = call(
                functools.partial(cell_kernel, step, False),
                [sent, cells, state_shape, cells, cells],
                6 + len(extra),
            )(recv, gt, g, vraw, alpha, state, *extra)
    recv = exchange(send)
    scale = float(BLK_DEV * width * ndev) ** 0.5
    (right,) = call(functools.partial(norm_kernel, scale), [cells], 2)(recv, vraw)
    return (solution, right)


def solution(mesh):
    split = Mesh(mesh.devices.reshape(4, 4, 4, 2), AXES)
    placed = (
        P(AXES, None, None),
        P(AXES, None),
        P(AXES),
        P(AXES),
        P(AXES),
        P(AXES, None, None),
    )
    return jax.shard_map(
        per_device,
        mesh=split,
        in_specs=placed,
        out_specs=(P(AXES, None), P(AXES, None)),
        check_vma=False,
    )
```

```python
import functools

import jax
import jax.numpy as jnp
from jax import lax
from jax.experimental import pallas as pl
from jax.experimental.pallas import tpu as pltpu
from jax.sharding import Mesh
from jax.sharding import PartitionSpec as P

BLK_DEV = 256
ITERS = 3
AXES = ("src_0", "src_1", "reg_0", "reg_1")
damping = 0.5

F32 = jnp.float32
BF16 = jnp.bfloat16
ROWS = 4
UNROLL = 128
CHUNK = 32
DEPTH = 4
FIRST_UNROLL = 64
PARTS = 2
EXTRA = 16


def iota(shape, axis):
    return lax.broadcasted_iota(jnp.int32, shape, axis)


def onehot(x):
    return x.astype(F32).astype(BF16)


def dot(a, b, dims=((1,), (0,))):
    return lax.dot_general(a, b, (dims, ((), ())), preferred_element_type=F32)


def exact_dot(matrix, x):
    hi = x.astype(BF16)
    lo = (x - hi.astype(F32)).astype(BF16)
    both = dot(matrix, jnp.concatenate([hi, lo], axis=1))
    width = x.shape[1]
    return both[:, :width] + both[:, width:]


def with_scalar(sums, x):
    a = x.astype(BF16).astype(F32)
    b = (x - a).astype(BF16).astype(F32)
    c = x - a - b
    lane = iota((1, 8, 128), 2)
    row = iota((1, 8, 128), 1) & (ROWS - 1)
    v = jnp.where(lane == 0, a, jnp.where(lane == 1, b, jnp.where(lane == 2, c, 0.0)))
    out = jnp.where(row == 2, v, sums.reshape(-1, 8, 128))
    return out.reshape(sums.shape).astype(BF16)


def scalar_total(row):
    return jnp.sum(jnp.where(iota((1, 128), 1) < 3, row, 0.0), axis=1, keepdims=True)


def received_total(recv):
    rows = jnp.sum(recv.astype(F32).reshape(-1, 8, 128), axis=0)
    scalar = (iota((8, 128), 0) & (ROWS - 1) == 2) & (iota((8, 128), 1) < 3)
    return total(jnp.where(scalar, rows, 0.0))


def total(x):
    return jnp.sum(jnp.sum(x, axis=0, keepdims=True), axis=1, keepdims=True)


def products(picked_ref, tiles_ref, out_ref, first, offset, number):
    row = iota((16, 128), 0)
    left = onehot((row & 1) == 0)
    right = 1 - left
    row8 = iota((8, 128), 0)
    low = row8 < 4
    side = (row8 & 3) < 2
    for pack in range(number // 16):
        base = first + 16 * pack
        pk = picked_ref[pl.ds(base + offset, 16), :]
        lhs = jnp.concatenate([pk * left, pk * right], axis=1)
        res = []
        for g in range(4):
            at = base + 4 * g
            wa = tiles_ref[pl.ds(at, 2)].reshape(256, 128)
            wb = tiles_ref[pl.ds(at + 2, 2)].reshape(256, 128)
            res.append(dot(lhs, jnp.concatenate([wa, wb], axis=1)))
        for h in range(2):
            a = res[2 * h][8 * h : 8 * h + 8]
            b = res[2 * h + 1][8 * h : 8 * h + 8]
            a = jnp.where(side, a[:, :128], a[:, 128:])
            b = jnp.where(side, b[:, :128], b[:, 128:])
            out_ref[pl.ds(base + offset + 8 * h, 8), :] = jnp.where(low, a, b)


def first_kernel(
    count_ref, tiles_ref, rays_ref, rows_ref, slots_ref, wanted_ref,
    *refs,
):
    tiles, turned, refs = refs[:PARTS], refs[PARTS : 2 * PARTS], refs[2 * PARTS :]
    send_ref, rays, st_ref, rt_ref, s_ref, r_ref, g_ref, gt_ref = refs[:8]
    rows, slots, wanted, picked, res, sem, small_sem = refs[8:]
    ntile = tiles_ref.shape[0]
    nrow = rays_ref.shape[0]
    nq = st_ref.shape[0]
    cap, ndev = wanted_ref.shape

    part = ntile // PARTS
    copies = part // CHUNK

    def copy(p, i):
        src = tiles_ref.at[pl.ds(p * part + i * CHUNK, CHUNK)]
        return pltpu.make_async_copy(src, tiles[p].at[pl.ds(i * CHUNK, CHUNK)], sem.at[p, i])

    pairs = ((rows_ref, rows), (rays_ref, rays), (slots_ref, slots), (wanted_ref, wanted))
    small = [pltpu.make_async_copy(a, b, small_sem.at[i]) for i, (a, b) in enumerate(pairs)]
    for c in small:
        c.start()
    for i in range(DEPTH):
        copy(0, i).start()
    for c in small:
        c.wait()
    live = iota((1, ntile), 1) < count_ref[0]
    row_of = jnp.where(live, rows[...], -1)
    slot_of = slots[...]
    slot_of = jnp.where(live, (slot_of >> 1) * ROWS + (slot_of & 1), -1)
    rt = onehot(jnp.broadcast_to(row_of, (nrow, ntile)) == iota((nrow, ntile), 0))
    rt_ref[...] = rt
    r_ref[...] = rt.T
    uraw = rays[...]
    picked[...] = dot(r_ref[...], uraw.astype(BF16)).astype(BF16)
    uu = total(uraw * uraw)
    for q in range(0, nq, 128):
        st = jnp.broadcast_to(slot_of, (128, ntile)) == iota((128, ntile), 0) + q
        st = onehot(st)
        st_ref[q : q + 128, :] = st
        s_ref[:ntile, q : q + 128] = st.T
    scalar = (iota((EXTRA, nq), 1) & (ROWS - 1) == 2) & (iota((EXTRA, nq), 0) == 0)
    scalar = onehot(scalar)
    s_ref[ntile:, :] = scalar
    req = wanted[...].astype(F32)
    q = iota((nq, ndev), 0)
    peer = q >> 2 == iota((nq, ndev), 1)
    value = jnp.zeros((nq, 128), F32)
    for c in range(cap):
        column = jnp.broadcast_to(req[c : c + 1, :], (128, ndev)).T.astype(BF16)
        value = value + dot(onehot(peer & (q & (ROWS - 1) == c)), column)
    value = jnp.where(iota((nq, 128), 0) & (ROWS - 1) < cap, value, -1.0)
    value = value.astype(jnp.int32)
    for b in range(0, BLK_DEV, 128):
        g = onehot(value == iota((nq, 128), 1) + b)
        g_ref[:, b : b + 128] = g
        gt_ref[b : b + 128, :] = g.T

    for p in range(PARTS):

        def body(i, carry):
            each = FIRST_UNROLL // CHUNK
            for j in range(each):
                n = i * each + j
                copy(p, n).wait()
                n = n + DEPTH

                @pl.when(n < copies)
                def _():
                    copy(p, n).start()

                if p + 1 < PARTS:

                    @pl.when(n >= copies)
                    def _():
                        copy(p + 1, n - copies).start()

            for j in range(FIRST_UNROLL):
                turned[p][i * FIRST_UNROLL + j] = tiles[p][i * FIRST_UNROLL + j].T
            products(picked, tiles[p], res, i * FIRST_UNROLL, p * part, FIRST_UNROLL)
            return carry

        lax.fori_loop(0, part // FIRST_UNROLL, body, 0)
    sums = exact_dot(st_ref[...], res[...])
    send_ref[...] = with_scalar(sums, uu)


def ray_kernel(*refs):
    tiles, turned, refs = refs[:PARTS], refs[PARTS : 2 * PARTS], refs[2 * PARTS :]
    recv_ref, s_ref, st_ref, r_ref, rt_ref, uraw_ref, beta_ref = refs[:7]
    send_ref, uraw_out, alpha_ref, picked, res = refs[7:]
    part = tiles[0].shape[0]
    ntile = PARTS * part

    def run(parts):
        for p in range(PARTS):

            def body(i, carry):
                products(picked, parts[p], res, i * UNROLL, p * part, UNROLL)
                return carry

            lax.fori_loop(0, part // UNROLL, body, 0)

    got = dot(s_ref[...], recv_ref[...])
    picked[...] = got[:ntile].astype(BF16)
    alpha = jnp.sqrt(scalar_total(got[ntile : ntile + 1]))

    run(turned)
    product = exact_dot(rt_ref[...], res[...])
    beta = beta_ref[0:1, 0:1]
    uraw = product / alpha - alpha * (uraw_ref[...] / beta)
    uraw_out[...] = uraw
    alpha_ref[...] = jnp.broadcast_to(alpha, (8, 128))
    picked[...] = dot(r_ref[...], uraw.astype(BF16)).astype(BF16)
    uu = total(uraw * uraw)

    run(tiles)
    sums = exact_dot(st_ref[...], res[...])
    send_ref[...] = with_scalar(sums, uu)


def cell_kernel(first, last, *refs):
    recv_ref, gt_ref = refs[:2]
    recv = recv_ref[...]
    beta = jnp.sqrt(received_total(recv))
    grad = dot(gt_ref[...], recv)
    send_ref, vraw_out, beta_out = refs[-3:]
    vraw = grad / beta
    if not first:
        vraw_ref, alpha_ref = refs[3:5]
        vraw = vraw - beta * (vraw_ref[...] / alpha_ref[0:1, 0:1])
    vraw_out[...] = vraw
    beta_out[...] = jnp.broadcast_to(beta, (8, 128))
    vv = total(vraw * vraw)
    if last:
        send_ref[...] = jnp.broadcast_to(vv, send_ref.shape)
    else:
        send_ref[...] = with_scalar(dot(refs[2][...], vraw.astype(BF16)), vv)


def last_kernel(scale, *refs):
    recv_ref = refs[0]
    vraws = refs[1 : ITERS + 2]
    alphas = [ref[0:1, 0:1] for ref in refs[ITERS + 2 : 2 * ITERS + 2]]
    betas = [ref[0:1, 0:1] for ref in refs[2 * ITERS + 2 : 3 * ITERS + 3]]
    solution_ref, right_ref = refs[3 * ITERS + 3 :]
    vv = jnp.sum(jnp.sum(recv_ref[...], axis=0, keepdims=True)[:, 0:1], axis=1, keepdims=True)
    right_ref[...] = vraws[ITERS][...] * (scale / jnp.sqrt(vv))
    w = vraws[0][...] / alphas[0]
    phibar = betas[0]
    rhobar = alphas[0]
    solution = None
    for step in range(1, ITERS + 1):
        beta = betas[step]
        rhobar1 = jnp.sqrt(rhobar * rhobar + damping * damping)
        phibar = rhobar / rhobar1 * phibar
        rho = jnp.sqrt(rhobar1 * rhobar1 + beta * beta)
        cosine = rhobar1 / rho
        sine = beta / rho
        phi = cosine * phibar
        phibar = sine * phibar
        update = (phi / rho) * w
        solution = update if solution is None else solution + update
        if step < ITERS:
            alpha = alphas[step]
            w = vraws[step][...] / alpha - (sine * alpha / rho) * w
            rhobar = -cosine * alpha
    solution_ref[...] = solution


def shape(dims, dtype=F32):
    return jax.ShapeDtypeStruct(dims, dtype)


VMEM = pl.BlockSpec(memory_space=pltpu.VMEM)
SMEM = pl.BlockSpec(memory_space=pltpu.SMEM)
HBM = pl.BlockSpec(memory_space=pltpu.HBM)


def call(kernel, outs, in_specs, scratch=(), limit=8 << 20):
    if isinstance(in_specs, int):
        in_specs = [VMEM] * in_specs
    return pl.pallas_call(
        kernel,
        out_shape=outs,
        in_specs=in_specs,
        out_specs=[VMEM] * len(outs),
        scratch_shapes=list(scratch),
        compiler_params=pltpu.CompilerParams(vmem_limit_bytes=limit),
    )


def per_device(tiles, rays, tile_rows, tile_slots, tile_count, wanted):
    ndev = lax.axis_size(AXES)
    ntile, _, width = tiles.shape
    nrow = rays.shape[0]
    nq = ndev * ROWS
    cap = wanted.shape[2]

    def exchange(x):
        rows = x.shape[0] // ndev
        y = lax.all_to_all(
            x.reshape(ndev, rows, width), AXES, split_axis=0, concat_axis=0, tiled=True
        )
        return y.reshape(x.shape)

    def far(x):
        return pltpu.with_memory_space_constraint(x, pltpu.HBM)

    cells = shape((BLK_DEV, width))
    scalar = shape((8, width))
    sent = shape((nq, width), BF16)
    scratch = [
        pltpu.VMEM((ntile, width), BF16),
        pltpu.VMEM((ntile, width), F32),
    ]
    *kept, send, uraw, st, rt, s, r, g, gt = call(
        first_kernel,
        [
            *[shape((ntile // PARTS, width, width), BF16)] * (2 * PARTS),
            sent,
            shape((nrow, width)),
            shape((nq, ntile), BF16),
            shape((nrow, ntile), BF16),
            shape((ntile + EXTRA, nq), BF16),
            shape((ntile, nrow), BF16),
            shape((nq, BLK_DEV), BF16),
            shape((BLK_DEV, nq), BF16),
        ],
        [SMEM] + [HBM] * 5,
        [
            pltpu.VMEM((1, ntile), jnp.int32),
            pltpu.VMEM((1, ntile), jnp.int32),
            pltpu.VMEM((cap, ndev), jnp.int32),
            *scratch,
            pltpu.SemaphoreType.DMA((PARTS, ntile // PARTS // CHUNK)),
            pltpu.SemaphoreType.DMA((4,)),
        ],
    )(
        tile_count,
        far(tiles),
        far(rays),
        far(tile_rows.reshape(1, ntile)),
        far(tile_slots.reshape(1, ntile)),
        far(wanted[0].T),
    )

    vraws, alphas, betas = [], [], []
    for step in range(ITERS + 1):
        last = step == ITERS
        if step > 0:
            recv = exchange(send)
            send, uraw, alpha = call(
                ray_kernel,
                [sent, shape((nrow, width)), scalar],
                2 * PARTS + 7,
                scratch,
            )(*kept, recv, s, st, r, rt, uraw, betas[-1])
            alphas.append(alpha)
        recv = exchange(send)
        prior = [] if step == 0 else [vraws[-1], alphas[-1]]
        send, vraw, beta = call(
            functools.partial(cell_kernel, step == 0, last),
            [shape((ndev, width)) if last else sent, cells, scalar],
            3 + len(prior),
        )(recv, gt, g, *prior)
        vraws.append(vraw)
        betas.append(beta)
    recv = exchange(send)
    scale = float(BLK_DEV * width * ndev) ** 0.5
    return tuple(
        call(functools.partial(last_kernel, scale), [cells, cells], 3 * ITERS + 3)(
            recv, *vraws, *alphas, *betas
        )
    )


def solution(mesh):
    split = Mesh(mesh.devices.reshape(4, 4, 4, 2), AXES)
    placed = (
        P(AXES, None, None),
        P(AXES, None),
        P(AXES),
        P(AXES),
        P(AXES),
        P(AXES, None, None),
    )
    return jax.shard_map(
        per_device,
        mesh=split,
        in_specs=placed,
        out_specs=(P(AXES, None), P(AXES, None)),
        check_vma=False,
    )
```

```python
import functools

import jax
import jax.numpy as jnp
from jax import lax
from jax.experimental import pallas as pl
from jax.experimental.pallas import tpu as pltpu
from jax.sharding import Mesh
from jax.sharding import PartitionSpec as P

BLK_DEV = 256
ITERS = 3
AXES = ("src_0", "src_1", "reg_0", "reg_1")
damping = 0.5

F32 = jnp.float32
BF16 = jnp.bfloat16
ROWS = 4
UNROLL = 128
CHUNK = 32
DEPTH = 6
FIRST_UNROLL = 64
PARTS = 2
EXTRA = 16


def iota(shape, axis):
    return lax.broadcasted_iota(jnp.int32, shape, axis)


def onehot(x):
    return x.astype(F32).astype(BF16)


def dot(a, b, dims=((1,), (0,))):
    return lax.dot_general(a, b, (dims, ((), ())), preferred_element_type=F32)


def exact_dot(matrix, x):
    hi = x.astype(BF16)
    lo = (x - hi.astype(F32)).astype(BF16)
    both = dot(matrix, jnp.concatenate([hi, lo], axis=1))
    width = x.shape[1]
    return both[:, :width] + both[:, width:]


def with_scalar(sums, x):
    a = x.astype(BF16).astype(F32)
    b = (x - a).astype(BF16).astype(F32)
    c = x - a - b
    lane = iota((1, 8, 128), 2)
    row = iota((1, 8, 128), 1) & (ROWS - 1)
    v = jnp.where(lane == 0, a, jnp.where(lane == 1, b, jnp.where(lane == 2, c, 0.0)))
    out = jnp.where(row == 2, v, sums.reshape(-1, 8, 128))
    return out.reshape(sums.shape).astype(BF16)


def scalar_total(row):
    return jnp.sum(jnp.where(iota((1, 128), 1) < 3, row, 0.0), axis=1, keepdims=True)


def received_total(recv):
    rows = jnp.sum(recv.astype(F32).reshape(-1, 8, 128), axis=0)
    scalar = (iota((8, 128), 0) & (ROWS - 1) == 2) & (iota((8, 128), 1) < 3)
    return total(jnp.where(scalar, rows, 0.0))


def total(x):
    return jnp.sum(jnp.sum(x, axis=0, keepdims=True), axis=1, keepdims=True)


def products(picked_ref, tiles_ref, out_ref, first, offset, number):
    row = iota((16, 128), 0)
    left = onehot((row & 1) == 0)
    right = 1 - left
    row8 = iota((8, 128), 0)
    low = row8 < 4
    side = (row8 & 3) < 2
    for pack in range(number // 16):
        base = first + 16 * pack
        pk = picked_ref[pl.ds(base + offset, 16), :]
        lhs = jnp.concatenate([pk * left, pk * right], axis=1)
        res = []
        for g in range(4):
            at = base + 4 * g
            wa = tiles_ref[pl.ds(at, 2)].reshape(256, 128)
            wb = tiles_ref[pl.ds(at + 2, 2)].reshape(256, 128)
            res.append(dot(lhs, jnp.concatenate([wa, wb], axis=1)))
        for h in range(2):
            a = res[2 * h][8 * h : 8 * h + 8]
            b = res[2 * h + 1][8 * h : 8 * h + 8]
            a = jnp.where(side, a[:, :128], a[:, 128:])
            b = jnp.where(side, b[:, :128], b[:, 128:])
            out_ref[pl.ds(base + offset + 8 * h, 8), :] = jnp.where(low, a, b)


def first_kernel(
    count_ref, tiles_ref, rays_ref, rows_ref, slots_ref, wanted_ref,
    *refs,
):
    tiles, turned, refs = refs[:PARTS], refs[PARTS : 2 * PARTS], refs[2 * PARTS :]
    send_ref, rays, st_ref, rt_ref, s_ref, r_ref, g_ref, gt_ref = refs[:8]
    rows, slots, wanted, picked, res, sem, small_sem = refs[8:]
    ntile = tiles_ref.shape[0]
    nrow = rays_ref.shape[0]
    nq = st_ref.shape[0]
    cap, ndev = wanted_ref.shape

    part = ntile // PARTS
    copies = part // CHUNK

    def copy(p, i):
        src = tiles_ref.at[pl.ds(p * part + i * CHUNK, CHUNK)]
        return pltpu.make_async_copy(src, tiles[p].at[pl.ds(i * CHUNK, CHUNK)], sem.at[p, i])

    pairs = ((rows_ref, rows), (rays_ref, rays), (slots_ref, slots), (wanted_ref, wanted))
    small = [pltpu.make_async_copy(a, b, small_sem.at[i]) for i, (a, b) in enumerate(pairs)]
    for c in small:
        c.start()
    for i in range(DEPTH):
        copy(0, i).start()
    for c in small:
        c.wait()
    live = iota((1, ntile), 1) < count_ref[0]
    row_of = jnp.where(live, rows[...], -1)
    slot_of = slots[...]
    slot_of = jnp.where(live, (slot_of >> 1) * ROWS + (slot_of & 1), -1)
    rt = onehot(jnp.broadcast_to(row_of, (nrow, ntile)) == iota((nrow, ntile), 0))
    rt_ref[...] = rt
    r_ref[...] = rt.T
    uraw = rays[...]
    picked[...] = dot(r_ref[...], uraw.astype(BF16)).astype(BF16)
    uu = total(uraw * uraw)
    for p in range(PARTS):
        for i in range(0, part, FIRST_UNROLL):
            for j in range(i // CHUNK, (i + FIRST_UNROLL) // CHUNK):
                copy(p, j).wait()
                n = p * copies + j + DEPTH
                if n < PARTS * copies:
                    copy(n // copies, n % copies).start()
            for j in range(i, i + FIRST_UNROLL):
                turned[p][j] = tiles[p][j].T
            products(picked, tiles[p], res, i, p * part, FIRST_UNROLL)
            if p == 0 and i == 0:
                for q in range(0, nq, 128):
                    st = jnp.broadcast_to(slot_of, (128, ntile)) == iota((128, ntile), 0) + q
                    st = onehot(st)
                    st_ref[q : q + 128, :] = st
                    s_ref[:ntile, q : q + 128] = st.T
                scalar = (iota((EXTRA, nq), 1) & (ROWS - 1) == 2) & (iota((EXTRA, nq), 0) == 0)
                scalar = onehot(scalar)
                s_ref[ntile:, :] = scalar
                req = wanted[...].astype(F32)
                q = iota((nq, ndev), 0)
                peer = q >> 2 == iota((nq, ndev), 1)
                value = jnp.zeros((nq, 128), F32)
                for c in range(cap):
                    column = jnp.broadcast_to(req[c : c + 1, :], (128, ndev)).T.astype(BF16)
                    value = value + dot(onehot(peer & (q & (ROWS - 1) == c)), column)
                value = jnp.where(iota((nq, 128), 0) & (ROWS - 1) < cap, value, -1.0)
                value = value.astype(jnp.int32)
                for b in range(0, BLK_DEV, 128):
                    g = onehot(value == iota((nq, 128), 1) + b)
                    g_ref[:, b : b + 128] = g
                    gt_ref[b : b + 128, :] = g.T
    sums = exact_dot(st_ref[...], res[...])
    send_ref[...] = with_scalar(sums, uu)


def ray_kernel(*refs):
    tiles, turned, refs = refs[:PARTS], refs[PARTS : 2 * PARTS], refs[2 * PARTS :]
    recv_ref, s_ref, st_ref, r_ref, rt_ref, uraw_ref, beta_ref = refs[:7]
    send_ref, uraw_out, alpha_ref, picked, res = refs[7:]
    part = tiles[0].shape[0]
    ntile = PARTS * part

    def run(parts):
        for p in range(PARTS):
            for i in range(0, part, UNROLL):
                products(picked, parts[p], res, i, p * part, UNROLL)

    got = dot(s_ref[...], recv_ref[...])
    picked[...] = got[:ntile].astype(BF16)
    alpha = jnp.sqrt(scalar_total(got[ntile : ntile + 1]))

    run(turned)
    product = exact_dot(rt_ref[...], res[...])
    beta = beta_ref[0:1, 0:1]
    uraw = product / alpha - alpha * (uraw_ref[...] / beta)
    uraw_out[...] = uraw
    alpha_ref[...] = jnp.broadcast_to(alpha, (8, 128))
    picked[...] = dot(r_ref[...], uraw.astype(BF16)).astype(BF16)
    uu = total(uraw * uraw)

    run(tiles)
    sums = exact_dot(st_ref[...], res[...])
    send_ref[...] = with_scalar(sums, uu)


def cell_kernel(first, last, *refs):
    recv_ref, gt_ref = refs[:2]
    recv = recv_ref[...]
    beta = jnp.sqrt(received_total(recv))
    grad = dot(gt_ref[...], recv)
    send_ref, vraw_out, beta_out = refs[-3:]
    vraw = grad / beta
    if not first:
        vraw_ref, alpha_ref = refs[3:5]
        vraw = vraw - beta * (vraw_ref[...] / alpha_ref[0:1, 0:1])
    vraw_out[...] = vraw
    beta_out[...] = jnp.broadcast_to(beta, (8, 128))
    vv = total(vraw * vraw)
    if last:
        send_ref[...] = jnp.broadcast_to(vv, send_ref.shape)
    else:
        send_ref[...] = with_scalar(dot(refs[2][...], vraw.astype(BF16)), vv)


def last_kernel(scale, *refs):
    recv_ref = refs[0]
    vraws = refs[1 : ITERS + 2]
    alphas = [ref[0:1, 0:1] for ref in refs[ITERS + 2 : 2 * ITERS + 2]]
    betas = [ref[0:1, 0:1] for ref in refs[2 * ITERS + 2 : 3 * ITERS + 3]]
    solution_ref, right_ref = refs[3 * ITERS + 3 :]
    vv = jnp.sum(jnp.sum(recv_ref[...], axis=0, keepdims=True)[:, 0:1], axis=1, keepdims=True)
    right_ref[...] = vraws[ITERS][...] * (scale / jnp.sqrt(vv))
    w = vraws[0][...] / alphas[0]
    phibar = betas[0]
    rhobar = alphas[0]
    solution = None
    for step in range(1, ITERS + 1):
        beta = betas[step]
        rhobar1 = jnp.sqrt(rhobar * rhobar + damping * damping)
        phibar = rhobar / rhobar1 * phibar
        rho = jnp.sqrt(rhobar1 * rhobar1 + beta * beta)
        cosine = rhobar1 / rho
        sine = beta / rho
        phi = cosine * phibar
        phibar = sine * phibar
        update = (phi / rho) * w
        solution = update if solution is None else solution + update
        if step < ITERS:
            alpha = alphas[step]
            w = vraws[step][...] / alpha - (sine * alpha / rho) * w
            rhobar = -cosine * alpha
    solution_ref[...] = solution


def shape(dims, dtype=F32):
    return jax.ShapeDtypeStruct(dims, dtype)


VMEM = pl.BlockSpec(memory_space=pltpu.VMEM)
SMEM = pl.BlockSpec(memory_space=pltpu.SMEM)
HBM = pl.BlockSpec(memory_space=pltpu.HBM)


def call(kernel, outs, in_specs, scratch=(), limit=8 << 20):
    if isinstance(in_specs, int):
        in_specs = [VMEM] * in_specs
    return pl.pallas_call(
        kernel,
        out_shape=outs,
        in_specs=in_specs,
        out_specs=[VMEM] * len(outs),
        scratch_shapes=list(scratch),
        compiler_params=pltpu.CompilerParams(vmem_limit_bytes=limit),
    )


def per_device(tiles, rays, tile_rows, tile_slots, tile_count, wanted):
    ndev = lax.axis_size(AXES)
    ntile, _, width = tiles.shape
    nrow = rays.shape[0]
    nq = ndev * ROWS
    cap = wanted.shape[2]

    def exchange(x):
        rows = x.shape[0] // ndev
        y = lax.all_to_all(
            x.reshape(ndev, rows, width), AXES, split_axis=0, concat_axis=0, tiled=True
        )
        return y.reshape(x.shape)

    def far(x):
        return pltpu.with_memory_space_constraint(x, pltpu.HBM)

    cells = shape((BLK_DEV, width))
    scalar = shape((8, width))
    sent = shape((nq, width), BF16)
    scratch = [
        pltpu.VMEM((ntile, width), BF16),
        pltpu.VMEM((ntile, width), F32),
    ]
    *kept, send, uraw, st, rt, s, r, g, gt = call(
        first_kernel,
        [
            *[shape((ntile // PARTS, width, width), BF16)] * (2 * PARTS),
            sent,
            shape((nrow, width)),
            shape((nq, ntile), BF16),
            shape((nrow, ntile), BF16),
            shape((ntile + EXTRA, nq), BF16),
            shape((ntile, nrow), BF16),
            shape((nq, BLK_DEV), BF16),
            shape((BLK_DEV, nq), BF16),
        ],
        [SMEM] + [HBM] * 5,
        [
            pltpu.VMEM((1, ntile), jnp.int32),
            pltpu.VMEM((1, ntile), jnp.int32),
            pltpu.VMEM((cap, ndev), jnp.int32),
            *scratch,
            pltpu.SemaphoreType.DMA((PARTS, ntile // PARTS // CHUNK)),
            pltpu.SemaphoreType.DMA((4,)),
        ],
    )(
        tile_count,
        far(tiles),
        far(rays),
        far(tile_rows.reshape(1, ntile)),
        far(tile_slots.reshape(1, ntile)),
        far(wanted[0].T),
    )

    vraws, alphas, betas = [], [], []
    for step in range(ITERS + 1):
        last = step == ITERS
        if step > 0:
            recv = exchange(send)
            send, uraw, alpha = call(
                ray_kernel,
                [sent, shape((nrow, width)), scalar],
                2 * PARTS + 7,
                scratch,
            )(*kept, recv, s, st, r, rt, uraw, betas[-1])
            alphas.append(alpha)
        recv = exchange(send)
        prior = [] if step == 0 else [vraws[-1], alphas[-1]]
        send, vraw, beta = call(
            functools.partial(cell_kernel, step == 0, last),
            [shape((ndev, width)) if last else sent, cells, scalar],
            3 + len(prior),
        )(recv, gt, g, *prior)
        vraws.append(vraw)
        betas.append(beta)
    recv = exchange(send)
    scale = float(BLK_DEV * width * ndev) ** 0.5
    return tuple(
        call(functools.partial(last_kernel, scale), [cells, cells], 3 * ITERS + 3)(
            recv, *vraws, *alphas, *betas
        )
    )


def solution(mesh):
    split = Mesh(mesh.devices.reshape(4, 4, 4, 2), AXES)
    placed = (
        P(AXES, None, None),
        P(AXES, None),
        P(AXES),
        P(AXES),
        P(AXES),
        P(AXES, None, None),
    )
    return jax.shard_map(
        per_device,
        mesh=split,
        in_specs=placed,
        out_specs=(P(AXES, None), P(AXES, None)),
        check_vma=False,
    )
```

```python
import functools

import jax
import jax.numpy as jnp
from jax import lax
from jax.experimental import pallas as pl
from jax.experimental.pallas import tpu as pltpu
from jax.sharding import Mesh
from jax.sharding import PartitionSpec as P

BLK_DEV = 256
ITERS = 3
AXES = ("src_0", "src_1", "reg_0", "reg_1")
damping = 0.5

F32 = jnp.float32
BF16 = jnp.bfloat16
ROWS = 4
UNROLL = 128
CHUNK = 32
DEPTH = 6
FIRST_UNROLL = 64
PARTS = 2
VECTOR = 4
EXTRA = 16


def iota(shape, axis):
    return lax.broadcasted_iota(jnp.int32, shape, axis)


def onehot(x):
    return x.astype(F32).astype(BF16)


def dot(a, b, dims=((1,), (0,))):
    return lax.dot_general(a, b, (dims, ((), ())), preferred_element_type=F32)


def exact_dot(matrix, x):
    hi = x.astype(BF16)
    lo = (x - hi.astype(F32)).astype(BF16)
    both = dot(matrix, jnp.concatenate([hi, lo], axis=1))
    width = x.shape[1]
    return both[:, :width] + both[:, width:]


def with_scalar(sums, x):
    a = x.astype(BF16).astype(F32)
    b = (x - a).astype(BF16).astype(F32)
    c = x - a - b
    lane = iota((1, 8, 128), 2)
    row = iota((1, 8, 128), 1) & (ROWS - 1)
    v = jnp.where(lane == 0, a, jnp.where(lane == 1, b, jnp.where(lane == 2, c, 0.0)))
    out = jnp.where(row == 2, v, sums.reshape(-1, 8, 128))
    return out.reshape(sums.shape).astype(BF16)


def scalar_total(row):
    return jnp.sum(jnp.where(iota((1, 128), 1) < 3, row, 0.0), axis=1, keepdims=True)


def received_total(recv):
    rows = jnp.sum(recv.astype(F32).reshape(-1, 8, 128), axis=0)
    scalar = (iota((8, 128), 0) & (ROWS - 1) == 2) & (iota((8, 128), 1) < 3)
    return total(jnp.where(scalar, rows, 0.0))


def total(x):
    return jnp.sum(jnp.sum(x, axis=0, keepdims=True), axis=1, keepdims=True)


def products(picked_ref, tiles_ref, out_ref, first, offset, number, vector=0):
    row = iota((16, 128), 0)
    left = onehot((row & 1) == 0)
    right = 1 - left
    row8 = iota((8, 128), 0)
    low = row8 < 4
    side = (row8 & 3) < 2
    columns = None
    if vector:
        columns = picked_ref[pl.ds(first + offset, number), :].T
    for pack in range(number // 16):
        base = first + 16 * pack
        pk = picked_ref[pl.ds(base + offset, 16), :]
        lhs = jnp.concatenate([pk * left, pk * right], axis=1)
        res = []
        for g in range(4 - vector // 4):
            at = base + 4 * g
            wa = tiles_ref[pl.ds(at, 2)].reshape(256, 128)
            wb = tiles_ref[pl.ds(at + 2, 2)].reshape(256, 128)
            res.append(dot(lhs, jnp.concatenate([wa, wb], axis=1)))
        for h in range(2):
            halves = []
            for g in (2 * h, 2 * h + 1):
                if g < len(res):
                    r = res[g][8 * h : 8 * h + 8]
                    halves.append(jnp.where(side, r[:, :128], r[:, 128:]))
                else:
                    rows = []
                    for j in range(4):
                        t = 16 * pack + 4 * g + j
                        column = jnp.broadcast_to(columns[:, t : t + 1], (128, 128))
                        product = column * tiles_ref[first + t]
                        for size in (64, 32, 16):
                            product = product[:size] + product[size:]
                        partial = product.astype(F32)
                        partial = partial[:8] + partial[8:]
                        rows.append(jnp.sum(partial, axis=0, keepdims=True))
                    value = jnp.broadcast_to(rows[3], (8, 128))
                    for j in range(3):
                        value = jnp.where((row8 & 3) == j, rows[j], value)
                    halves.append(value)
            out_ref[pl.ds(base + offset + 8 * h, 8), :] = jnp.where(low, *halves)


def first_kernel(
    count_ref, tiles_ref, rays_ref, rows_ref, slots_ref, wanted_ref,
    *refs,
):
    tiles, turned, refs = refs[:PARTS], refs[PARTS : 2 * PARTS], refs[2 * PARTS :]
    send_ref, rays, st_ref, rt_ref, s_ref, r_ref, g_ref, gt_ref = refs[:8]
    rows, slots, wanted, picked, res, sem, small_sem = refs[8:]
    ntile = tiles_ref.shape[0]
    nrow = rays_ref.shape[0]
    nq = st_ref.shape[0]
    cap, ndev = wanted_ref.shape

    part = ntile // PARTS
    copies = part // CHUNK

    def copy(p, i):
        src = tiles_ref.at[pl.ds(p * part + i * CHUNK, CHUNK)]
        return pltpu.make_async_copy(src, tiles[p].at[pl.ds(i * CHUNK, CHUNK)], sem.at[p, i])

    pairs = ((rows_ref, rows), (rays_ref, rays), (slots_ref, slots), (wanted_ref, wanted))
    small = [pltpu.make_async_copy(a, b, small_sem.at[i]) for i, (a, b) in enumerate(pairs)]
    for c in small:
        c.start()
    for i in range(DEPTH):
        copy(0, i).start()
    for c in small:
        c.wait()
    live = iota((1, ntile), 1) < count_ref[0]
    row_of = jnp.where(live, rows[...], -1)
    slot_of = slots[...]
    slot_of = jnp.where(live, (slot_of >> 1) * ROWS + (slot_of & 1), -1)
    rt = onehot(jnp.broadcast_to(row_of, (nrow, ntile)) == iota((nrow, ntile), 0))
    rt_ref[...] = rt
    r_ref[...] = rt.T
    uraw = rays[...]
    picked[...] = dot(r_ref[...], uraw.astype(BF16)).astype(BF16)
    uu = total(uraw * uraw)
    for p in range(PARTS):
        for i in range(0, part, FIRST_UNROLL):
            for j in range(i // CHUNK, (i + FIRST_UNROLL) // CHUNK):
                copy(p, j).wait()
                n = p * copies + j + DEPTH
                if n < PARTS * copies:
                    copy(n // copies, n % copies).start()
            for j in range(i, i + FIRST_UNROLL):
                turned[p][j] = tiles[p][j].T
            products(picked, tiles[p], res, i, p * part, FIRST_UNROLL)
            if p == 0 and i == 0:
                for q in range(0, nq, 128):
                    st = jnp.broadcast_to(slot_of, (128, ntile)) == iota((128, ntile), 0) + q
                    st = onehot(st)
                    st_ref[q : q + 128, :] = st
                    s_ref[:ntile, q : q + 128] = st.T
                scalar = (iota((EXTRA, nq), 1) & (ROWS - 1) == 2) & (iota((EXTRA, nq), 0) == 0)
                scalar = onehot(scalar)
                s_ref[ntile:, :] = scalar
                req = wanted[...].astype(F32)
                q = iota((nq, ndev), 0)
                peer = q >> 2 == iota((nq, ndev), 1)
                value = jnp.zeros((nq, 128), F32)
                for c in range(cap):
                    column = jnp.broadcast_to(req[c : c + 1, :], (128, ndev)).T.astype(BF16)
                    value = value + dot(onehot(peer & (q & (ROWS - 1) == c)), column)
                value = jnp.where(iota((nq, 128), 0) & (ROWS - 1) < cap, value, -1.0)
                value = value.astype(jnp.int32)
                for b in range(0, BLK_DEV, 128):
                    g = onehot(value == iota((nq, 128), 1) + b)
                    g_ref[:, b : b + 128] = g
                    gt_ref[b : b + 128, :] = g.T
    sums = exact_dot(st_ref[...], res[...])
    send_ref[...] = with_scalar(sums, uu)


def ray_kernel(*refs):
    tiles, turned, refs = refs[:PARTS], refs[PARTS : 2 * PARTS], refs[2 * PARTS :]
    recv_ref, s_ref, st_ref, r_ref, rt_ref, uraw_ref, beta_ref = refs[:7]
    send_ref, uraw_out, alpha_ref, picked, res = refs[7:]
    part = tiles[0].shape[0]
    ntile = PARTS * part

    def run(parts):
        for p in range(PARTS):
            for i in range(0, part, UNROLL):
                products(picked, parts[p], res, i, p * part, UNROLL, VECTOR)

    got = dot(s_ref[...], recv_ref[...])
    picked[...] = got[:ntile].astype(BF16)
    alpha = jnp.sqrt(scalar_total(got[ntile : ntile + 1]))

    run(turned)
    product = exact_dot(rt_ref[...], res[...])
    beta = beta_ref[0:1, 0:1]
    uraw = product / alpha - alpha * (uraw_ref[...] / beta)
    uraw_out[...] = uraw
    alpha_ref[...] = jnp.broadcast_to(alpha, (8, 128))
    picked[...] = dot(r_ref[...], uraw.astype(BF16)).astype(BF16)
    uu = total(uraw * uraw)

    run(tiles)
    sums = exact_dot(st_ref[...], res[...])
    send_ref[...] = with_scalar(sums, uu)


def cell_kernel(first, last, *refs):
    recv_ref, gt_ref = refs[:2]
    recv = recv_ref[...]
    beta = jnp.sqrt(received_total(recv))
    grad = dot(gt_ref[...], recv)
    send_ref, vraw_out, beta_out = refs[-3:]
    vraw = grad / beta
    if not first:
        vraw_ref, alpha_ref = refs[3:5]
        vraw = vraw - beta * (vraw_ref[...] / alpha_ref[0:1, 0:1])
    vraw_out[...] = vraw
    beta_out[...] = jnp.broadcast_to(beta, (8, 128))
    vv = total(vraw * vraw)
    if last:
        send_ref[...] = jnp.broadcast_to(vv, send_ref.shape)
    else:
        send_ref[...] = with_scalar(dot(refs[2][...], vraw.astype(BF16)), vv)


def last_kernel(scale, *refs):
    recv_ref = refs[0]
    vraws = refs[1 : ITERS + 2]
    alphas = [ref[0:1, 0:1] for ref in refs[ITERS + 2 : 2 * ITERS + 2]]
    betas = [ref[0:1, 0:1] for ref in refs[2 * ITERS + 2 : 3 * ITERS + 3]]
    solution_ref, right_ref = refs[3 * ITERS + 3 :]
    vv = jnp.sum(jnp.sum(recv_ref[...], axis=0, keepdims=True)[:, 0:1], axis=1, keepdims=True)
    right_ref[...] = vraws[ITERS][...] * (scale / jnp.sqrt(vv))
    w = vraws[0][...] / alphas[0]
    phibar = betas[0]
    rhobar = alphas[0]
    solution = None
    for step in range(1, ITERS + 1):
        beta = betas[step]
        rhobar1 = jnp.sqrt(rhobar * rhobar + damping * damping)
        phibar = rhobar / rhobar1 * phibar
        rho = jnp.sqrt(rhobar1 * rhobar1 + beta * beta)
        cosine = rhobar1 / rho
        sine = beta / rho
        phi = cosine * phibar
        phibar = sine * phibar
        update = (phi / rho) * w
        solution = update if solution is None else solution + update
        if step < ITERS:
            alpha = alphas[step]
            w = vraws[step][...] / alpha - (sine * alpha / rho) * w
            rhobar = -cosine * alpha
    solution_ref[...] = solution


def shape(dims, dtype=F32):
    return jax.ShapeDtypeStruct(dims, dtype)


VMEM = pl.BlockSpec(memory_space=pltpu.VMEM)
SMEM = pl.BlockSpec(memory_space=pltpu.SMEM)
HBM = pl.BlockSpec(memory_space=pltpu.HBM)


def call(kernel, outs, in_specs, scratch=(), limit=8 << 20):
    if isinstance(in_specs, int):
        in_specs = [VMEM] * in_specs
    return pl.pallas_call(
        kernel,
        out_shape=outs,
        in_specs=in_specs,
        out_specs=[VMEM] * len(outs),
        scratch_shapes=list(scratch),
        compiler_params=pltpu.CompilerParams(vmem_limit_bytes=limit),
    )


def per_device(tiles, rays, tile_rows, tile_slots, tile_count, wanted):
    ndev = lax.axis_size(AXES)
    ntile, _, width = tiles.shape
    nrow = rays.shape[0]
    nq = ndev * ROWS
    cap = wanted.shape[2]

    def exchange(x):
        rows = x.shape[0] // ndev
        y = lax.all_to_all(
            x.reshape(ndev, rows, width), AXES, split_axis=0, concat_axis=0, tiled=True
        )
        return y.reshape(x.shape)

    def far(x):
        return pltpu.with_memory_space_constraint(x, pltpu.HBM)

    cells = shape((BLK_DEV, width))
    scalar = shape((8, width))
    sent = shape((nq, width), BF16)
    scratch = [
        pltpu.VMEM((ntile, width), BF16),
        pltpu.VMEM((ntile, width), F32),
    ]
    *kept, send, uraw, st, rt, s, r, g, gt = call(
        first_kernel,
        [
            *[shape((ntile // PARTS, width, width), BF16)] * (2 * PARTS),
            sent,
            shape((nrow, width)),
            shape((nq, ntile), BF16),
            shape((nrow, ntile), BF16),
            shape((ntile + EXTRA, nq), BF16),
            shape((ntile, nrow), BF16),
            shape((nq, BLK_DEV), BF16),
            shape((BLK_DEV, nq), BF16),
        ],
        [SMEM] + [HBM] * 5,
        [
            pltpu.VMEM((1, ntile), jnp.int32),
            pltpu.VMEM((1, ntile), jnp.int32),
            pltpu.VMEM((cap, ndev), jnp.int32),
            *scratch,
            pltpu.SemaphoreType.DMA((PARTS, ntile // PARTS // CHUNK)),
            pltpu.SemaphoreType.DMA((4,)),
        ],
    )(
        tile_count,
        far(tiles),
        far(rays),
        far(tile_rows.reshape(1, ntile)),
        far(tile_slots.reshape(1, ntile)),
        far(wanted[0].T),
    )

    vraws, alphas, betas = [], [], []
    for step in range(ITERS + 1):
        last = step == ITERS
        if step > 0:
            recv = exchange(send)
            send, uraw, alpha = call(
                ray_kernel,
                [sent, shape((nrow, width)), scalar],
                2 * PARTS + 7,
                scratch,
            )(*kept, recv, s, st, r, rt, uraw, betas[-1])
            alphas.append(alpha)
        recv = exchange(send)
        prior = [] if step == 0 else [vraws[-1], alphas[-1]]
        send, vraw, beta = call(
            functools.partial(cell_kernel, step == 0, last),
            [shape((ndev, width)) if last else sent, cells, scalar],
            3 + len(prior),
        )(recv, gt, g, *prior)
        vraws.append(vraw)
        betas.append(beta)
    recv = exchange(send)
    scale = float(BLK_DEV * width * ndev) ** 0.5
    return tuple(
        call(functools.partial(last_kernel, scale), [cells, cells], 3 * ITERS + 3)(
            recv, *vraws, *alphas, *betas
        )
    )


def solution(mesh):
    split = Mesh(mesh.devices.reshape(4, 4, 4, 2), AXES)
    placed = (
        P(AXES, None, None),
        P(AXES, None),
        P(AXES),
        P(AXES),
        P(AXES),
        P(AXES, None, None),
    )
    return jax.shard_map(
        per_device,
        mesh=split,
        in_specs=placed,
        out_specs=(P(AXES, None), P(AXES, None)),
        check_vma=False,
    )
```

```python
import functools

import jax
import jax.numpy as jnp
from jax import lax
from jax.experimental import pallas as pl
from jax.experimental.pallas import tpu as pltpu
from jax.sharding import Mesh
from jax.sharding import PartitionSpec as P

BLK_DEV = 256
ITERS = 3
AXES = ("src_0", "src_1", "reg_0", "reg_1")
damping = 0.5

F32 = jnp.float32
BF16 = jnp.bfloat16
ROWS = 4
UNROLL = 128
CHUNK = 32
DEPTH = 8
AHEAD = 2
FIRST_UNROLL = 64
PARTS = 2
VECTOR = 4
EXTRA = 16


def iota(shape, axis):
    return lax.broadcasted_iota(jnp.int32, shape, axis)


def onehot(x):
    return x.astype(F32).astype(BF16)


def dot(a, b, dims=((1,), (0,))):
    return lax.dot_general(a, b, (dims, ((), ())), preferred_element_type=F32)


def exact_dot(matrix, x):
    hi = x.astype(BF16)
    lo = (x - hi.astype(F32)).astype(BF16)
    both = dot(matrix, jnp.concatenate([hi, lo], axis=1))
    width = x.shape[1]
    return both[:, :width] + both[:, width:]


def with_scalar(sums, x):
    a = x.astype(BF16).astype(F32)
    b = (x - a).astype(BF16).astype(F32)
    c = x - a - b
    lane = iota((1, 8, 128), 2)
    row = iota((1, 8, 128), 1) & (ROWS - 1)
    v = jnp.where(lane == 0, a, jnp.where(lane == 1, b, jnp.where(lane == 2, c, 0.0)))
    out = jnp.where(row == 2, v, sums.reshape(-1, 8, 128))
    return out.reshape(sums.shape).astype(BF16)


def scalar_total(row):
    return jnp.sum(jnp.where(iota((1, 128), 1) < 3, row, 0.0), axis=1, keepdims=True)


def received_total(recv):
    rows = jnp.sum(recv.astype(F32).reshape(-1, 8, 128), axis=0)
    scalar = (iota((8, 128), 0) & (ROWS - 1) == 2) & (iota((8, 128), 1) < 3)
    return total(jnp.where(scalar, rows, 0.0))


def total(x):
    return jnp.sum(jnp.sum(x, axis=0, keepdims=True), axis=1, keepdims=True)


def products(picked_ref, tiles_ref, out_ref, first, offset, number, vector=0):
    row = iota((16, 128), 0)
    left = onehot((row & 1) == 0)
    right = 1 - left
    row8 = iota((8, 128), 0)
    low = row8 < 4
    side = (row8 & 3) < 2
    columns = None
    if vector:
        columns = picked_ref[pl.ds(first + offset, number), :].T
    for pack in range(number // 16):
        base = first + 16 * pack
        pk = picked_ref[pl.ds(base + offset, 16), :]
        lhs = jnp.concatenate([pk * left, pk * right], axis=1)
        res = []
        for g in range(4 - vector // 4):
            at = base + 4 * g
            wa = tiles_ref[pl.ds(at, 2)].reshape(256, 128)
            wb = tiles_ref[pl.ds(at + 2, 2)].reshape(256, 128)
            res.append(dot(lhs, jnp.concatenate([wa, wb], axis=1)))
        for h in range(2):
            halves = []
            for g in (2 * h, 2 * h + 1):
                if g < len(res):
                    r = res[g][8 * h : 8 * h + 8]
                    halves.append(jnp.where(side, r[:, :128], r[:, 128:]))
                else:
                    rows = []
                    for j in range(4):
                        t = 16 * pack + 4 * g + j
                        column = jnp.broadcast_to(columns[:, t : t + 1], (128, 128))
                        product = column * tiles_ref[first + t]
                        for size in (64, 32, 16):
                            product = product[:size] + product[size:]
                        partial = product.astype(F32)
                        partial = partial[:8] + partial[8:]
                        rows.append(jnp.sum(partial, axis=0, keepdims=True))
                    value = jnp.broadcast_to(rows[3], (8, 128))
                    for j in range(3):
                        value = jnp.where((row8 & 3) == j, rows[j], value)
                    halves.append(value)
            out_ref[pl.ds(base + offset + 8 * h, 8), :] = jnp.where(low, *halves)


def first_kernel(
    count_ref, tiles_ref, rays_ref, rows_ref, slots_ref, wanted_ref,
    *refs,
):
    tiles, turned, refs = refs[:PARTS], refs[PARTS : 2 * PARTS], refs[2 * PARTS :]
    send_ref, rays, st_ref, rt_ref, s_ref, r_ref, g_ref, gt_ref = refs[:8]
    rows, slots, wanted, picked, res, sem, small_sem = refs[8:]
    ntile = tiles_ref.shape[0]
    nrow = rays_ref.shape[0]
    nq = st_ref.shape[0]
    cap, ndev = wanted_ref.shape

    part = ntile // PARTS
    copies = part // CHUNK

    def copy(p, i):
        src = tiles_ref.at[pl.ds(p * part + i * CHUNK, CHUNK)]
        return pltpu.make_async_copy(src, tiles[p].at[pl.ds(i * CHUNK, CHUNK)], sem.at[p, i])

    pairs = ((rows_ref, rows), (rays_ref, rays), (slots_ref, slots), (wanted_ref, wanted))
    small = [pltpu.make_async_copy(a, b, small_sem.at[i]) for i, (a, b) in enumerate(pairs)]
    for c in small:
        c.start()
    for i in range(AHEAD):
        copy(0, i).start()
    for c in small:
        c.wait()
    live = iota((1, ntile), 1) < count_ref[0]
    row_of = jnp.where(live, rows[...], -1)
    slot_of = slots[...]
    slot_of = jnp.where(live, (slot_of >> 1) * ROWS + (slot_of & 1), -1)
    rt = onehot(jnp.broadcast_to(row_of, (nrow, ntile)) == iota((nrow, ntile), 0))
    rt_ref[...] = rt
    r_ref[...] = rt.T
    uraw = rays[...]
    picked[...] = dot(r_ref[...], uraw.astype(BF16)).astype(BF16)
    uu = total(uraw * uraw)
    for i in range(AHEAD, DEPTH):
        copy(0, i).start()
    for p in range(PARTS):
        for i in range(0, part, FIRST_UNROLL):
            for j in range(i // CHUNK, (i + FIRST_UNROLL) // CHUNK):
                copy(p, j).wait()
                n = p * copies + j + DEPTH
                if n < PARTS * copies:
                    copy(n // copies, n % copies).start()
            for j in range(i, i + FIRST_UNROLL):
                turned[p][j] = tiles[p][j].T
            products(picked, tiles[p], res, i, p * part, FIRST_UNROLL)
            if p == 0 and i == 0:
                for q in range(0, nq, 128):
                    st = jnp.broadcast_to(slot_of, (128, ntile)) == iota((128, ntile), 0) + q
                    st = onehot(st)
                    st_ref[q : q + 128, :] = st
                    s_ref[:ntile, q : q + 128] = st.T
                scalar = (iota((EXTRA, nq), 1) & (ROWS - 1) == 2) & (iota((EXTRA, nq), 0) == 0)
                scalar = onehot(scalar)
                s_ref[ntile:, :] = scalar
                req = wanted[...].astype(F32)
                q = iota((nq, ndev), 0)
                peer = q >> 2 == iota((nq, ndev), 1)
                value = jnp.zeros((nq, 128), F32)
                for c in range(cap):
                    column = jnp.broadcast_to(req[c : c + 1, :], (128, ndev)).T.astype(BF16)
                    value = value + dot(onehot(peer & (q & (ROWS - 1) == c)), column)
                value = jnp.where(iota((nq, 128), 0) & (ROWS - 1) < cap, value, -1.0)
                value = value.astype(jnp.int32)
                for b in range(0, BLK_DEV, 128):
                    g = onehot(value == iota((nq, 128), 1) + b)
                    g_ref[:, b : b + 128] = g
                    gt_ref[b : b + 128, :] = g.T
    sums = exact_dot(st_ref[...], res[...])
    send_ref[...] = with_scalar(sums, uu)


def ray_kernel(*refs):
    tiles, turned, refs = refs[:PARTS], refs[PARTS : 2 * PARTS], refs[2 * PARTS :]
    recv_ref, s_ref, st_ref, r_ref, rt_ref, uraw_ref, beta_ref = refs[:7]
    send_ref, uraw_out, alpha_ref, picked, res = refs[7:]
    part = tiles[0].shape[0]
    ntile = PARTS * part

    def run(parts):
        for p in range(PARTS):
            for i in range(0, part, UNROLL):
                products(picked, parts[p], res, i, p * part, UNROLL, VECTOR)

    got = dot(s_ref[...], recv_ref[...])
    picked[...] = got[:ntile].astype(BF16)
    alpha = jnp.sqrt(scalar_total(got[ntile : ntile + 1]))

    run(turned)
    product = exact_dot(rt_ref[...], res[...])
    beta = beta_ref[0:1, 0:1]
    uraw = product / alpha - alpha * (uraw_ref[...] / beta)
    uraw_out[...] = uraw
    alpha_ref[...] = jnp.broadcast_to(alpha, (8, 128))
    picked[...] = dot(r_ref[...], uraw.astype(BF16)).astype(BF16)
    uu = total(uraw * uraw)

    run(tiles)
    sums = exact_dot(st_ref[...], res[...])
    send_ref[...] = with_scalar(sums, uu)


def cell_kernel(first, last, *refs):
    recv_ref, gt_ref = refs[:2]
    recv = recv_ref[...]
    beta = jnp.sqrt(received_total(recv))
    grad = dot(gt_ref[...], recv)
    send_ref, vraw_out, beta_out = refs[-3:]
    vraw = grad / beta
    if not first:
        vraw_ref, alpha_ref = refs[3:5]
        vraw = vraw - beta * (vraw_ref[...] / alpha_ref[0:1, 0:1])
    vraw_out[...] = vraw
    beta_out[...] = jnp.broadcast_to(beta, (8, 128))
    vv = total(vraw * vraw)
    if last:
        send_ref[...] = jnp.broadcast_to(vv, send_ref.shape)
    else:
        send_ref[...] = with_scalar(dot(refs[2][...], vraw.astype(BF16)), vv)


def last_kernel(scale, *refs):
    recv_ref = refs[0]
    vraws = refs[1 : ITERS + 2]
    alphas = [ref[0:1, 0:1] for ref in refs[ITERS + 2 : 2 * ITERS + 2]]
    betas = [ref[0:1, 0:1] for ref in refs[2 * ITERS + 2 : 3 * ITERS + 3]]
    solution_ref, right_ref = refs[3 * ITERS + 3 :]
    vv = jnp.sum(jnp.sum(recv_ref[...], axis=0, keepdims=True)[:, 0:1], axis=1, keepdims=True)
    right_ref[...] = vraws[ITERS][...] * (scale / jnp.sqrt(vv))
    w = vraws[0][...] / alphas[0]
    phibar = betas[0]
    rhobar = alphas[0]
    solution = None
    for step in range(1, ITERS + 1):
        beta = betas[step]
        rhobar1 = jnp.sqrt(rhobar * rhobar + damping * damping)
        phibar = rhobar / rhobar1 * phibar
        rho = jnp.sqrt(rhobar1 * rhobar1 + beta * beta)
        cosine = rhobar1 / rho
        sine = beta / rho
        phi = cosine * phibar
        phibar = sine * phibar
        update = (phi / rho) * w
        solution = update if solution is None else solution + update
        if step < ITERS:
            alpha = alphas[step]
            w = vraws[step][...] / alpha - (sine * alpha / rho) * w
            rhobar = -cosine * alpha
    solution_ref[...] = solution


def shape(dims, dtype=F32):
    return jax.ShapeDtypeStruct(dims, dtype)


VMEM = pl.BlockSpec(memory_space=pltpu.VMEM)
SMEM = pl.BlockSpec(memory_space=pltpu.SMEM)
HBM = pl.BlockSpec(memory_space=pltpu.HBM)


def call(kernel, outs, in_specs, scratch=(), limit=8 << 20):
    if isinstance(in_specs, int):
        in_specs = [VMEM] * in_specs
    return pl.pallas_call(
        kernel,
        out_shape=outs,
        in_specs=in_specs,
        out_specs=[VMEM] * len(outs),
        scratch_shapes=list(scratch),
        compiler_params=pltpu.CompilerParams(vmem_limit_bytes=limit),
    )


def per_device(tiles, rays, tile_rows, tile_slots, tile_count, wanted):
    ndev = lax.axis_size(AXES)
    ntile, _, width = tiles.shape
    nrow = rays.shape[0]
    nq = ndev * ROWS
    cap = wanted.shape[2]

    def exchange(x):
        rows = x.shape[0] // ndev
        y = lax.all_to_all(
            x.reshape(ndev, rows, width), AXES, split_axis=0, concat_axis=0, tiled=True
        )
        return y.reshape(x.shape)

    def far(x):
        return pltpu.with_memory_space_constraint(x, pltpu.HBM)

    cells = shape((BLK_DEV, width))
    scalar = shape((8, width))
    sent = shape((nq, width), BF16)
    scratch = [
        pltpu.VMEM((ntile, width), BF16),
        pltpu.VMEM((ntile, width), F32),
    ]
    *kept, send, uraw, st, rt, s, r, g, gt = call(
        first_kernel,
        [
            *[shape((ntile // PARTS, width, width), BF16)] * (2 * PARTS),
            sent,
            shape((nrow, width)),
            shape((nq, ntile), BF16),
            shape((nrow, ntile), BF16),
            shape((ntile + EXTRA, nq), BF16),
            shape((ntile, nrow), BF16),
            shape((nq, BLK_DEV), BF16),
            shape((BLK_DEV, nq), BF16),
        ],
        [SMEM] + [HBM] * 5,
        [
            pltpu.VMEM((1, ntile), jnp.int32),
            pltpu.VMEM((1, ntile), jnp.int32),
            pltpu.VMEM((cap, ndev), jnp.int32),
            *scratch,
            pltpu.SemaphoreType.DMA((PARTS, ntile // PARTS // CHUNK)),
            pltpu.SemaphoreType.DMA((4,)),
        ],
    )(
        tile_count,
        far(tiles),
        far(rays),
        far(tile_rows.reshape(1, ntile)),
        far(tile_slots.reshape(1, ntile)),
        far(wanted[0].T),
    )

    vraws, alphas, betas = [], [], []
    for step in range(ITERS + 1):
        last = step == ITERS
        if step > 0:
            recv = exchange(send)
            send, uraw, alpha = call(
                ray_kernel,
                [sent, shape((nrow, width)), scalar],
                2 * PARTS + 7,
                scratch,
            )(*kept, recv, s, st, r, rt, uraw, betas[-1])
            alphas.append(alpha)
        recv = exchange(send)
        prior = [] if step == 0 else [vraws[-1], alphas[-1]]
        send, vraw, beta = call(
            functools.partial(cell_kernel, step == 0, last),
            [shape((ndev, width)) if last else sent, cells, scalar],
            3 + len(prior),
        )(recv, gt, g, *prior)
        vraws.append(vraw)
        betas.append(beta)
    recv = exchange(send)
    scale = float(BLK_DEV * width * ndev) ** 0.5
    return tuple(
        call(functools.partial(last_kernel, scale), [cells, cells], 3 * ITERS + 3)(
            recv, *vraws, *alphas, *betas
        )
    )


def solution(mesh):
    split = Mesh(mesh.devices.reshape(4, 4, 4, 2), AXES)
    placed = (
        P(AXES, None, None),
        P(AXES, None),
        P(AXES),
        P(AXES),
        P(AXES),
        P(AXES, None, None),
    )
    return jax.shard_map(
        per_device,
        mesh=split,
        in_specs=placed,
        out_specs=(P(AXES, None), P(AXES, None)),
        check_vma=False,
    )
```

```python
import functools

import jax
import jax.numpy as jnp
from jax import lax
from jax.experimental import pallas as pl
from jax.experimental.pallas import tpu as pltpu
from jax.sharding import Mesh
from jax.sharding import PartitionSpec as P

BLK_DEV = 256
ITERS = 3
AXES = ("src_0", "src_1", "reg_0", "reg_1")
damping = 0.5

F32 = jnp.float32
BF16 = jnp.bfloat16
ROWS = 4
UNROLL = 128
CHUNK = 32
DEPTH = 8
AHEAD = 2
GROUPS = (((0, 64), (64, 64), (128, 128)), ((0, 128), (128, 64), (192, 64)))
PARTS = 2
VECTOR = 4
EXTRA = 16


def iota(shape, axis):
    return lax.broadcasted_iota(jnp.int32, shape, axis)


def onehot(x):
    return x.astype(F32).astype(BF16)


def dot(a, b, dims=((1,), (0,))):
    return lax.dot_general(a, b, (dims, ((), ())), preferred_element_type=F32)


def exact_dot(matrix, x):
    hi = x.astype(BF16)
    lo = (x - hi.astype(F32)).astype(BF16)
    both = dot(matrix, jnp.concatenate([hi, lo], axis=1))
    width = x.shape[1]
    return both[:, :width] + both[:, width:]


def with_scalar(sums, x):
    a = x.astype(BF16).astype(F32)
    b = (x - a).astype(BF16).astype(F32)
    c = x - a - b
    lane = iota((1, 8, 128), 2)
    row = iota((1, 8, 128), 1) & (ROWS - 1)
    v = jnp.where(lane == 0, a, jnp.where(lane == 1, b, jnp.where(lane == 2, c, 0.0)))
    out = jnp.where(row == 2, v, sums.reshape(-1, 8, 128))
    return out.reshape(sums.shape).astype(BF16)


def scalar_total(row):
    return jnp.sum(jnp.where(iota((1, 128), 1) < 3, row, 0.0), axis=1, keepdims=True)


def received_total(recv):
    rows = jnp.sum(recv.astype(F32).reshape(-1, 8, 128), axis=0)
    scalar = (iota((8, 128), 0) & (ROWS - 1) == 2) & (iota((8, 128), 1) < 3)
    return total(jnp.where(scalar, rows, 0.0))


def total(x):
    return jnp.sum(jnp.sum(x, axis=0, keepdims=True), axis=1, keepdims=True)


def products(picked_ref, tiles_ref, out_ref, first, offset, number, vector=0):
    row = iota((16, 128), 0)
    left = onehot((row & 1) == 0)
    right = 1 - left
    row8 = iota((8, 128), 0)
    low = row8 < 4
    side = (row8 & 3) < 2
    columns = None
    if vector:
        columns = picked_ref[pl.ds(first + offset, number), :].T
    for pack in range(number // 16):
        base = first + 16 * pack
        pk = picked_ref[pl.ds(base + offset, 16), :]
        lhs = jnp.concatenate([pk * left, pk * right], axis=1)
        res = []
        for g in range(4 - vector // 4):
            at = base + 4 * g
            wa = tiles_ref[pl.ds(at, 2)].reshape(256, 128)
            wb = tiles_ref[pl.ds(at + 2, 2)].reshape(256, 128)
            res.append(dot(lhs, jnp.concatenate([wa, wb], axis=1)))
        for h in range(2):
            halves = []
            for g in (2 * h, 2 * h + 1):
                if g < len(res):
                    r = res[g][8 * h : 8 * h + 8]
                    halves.append(jnp.where(side, r[:, :128], r[:, 128:]))
                else:
                    rows = []
                    for j in range(4):
                        t = 16 * pack + 4 * g + j
                        column = jnp.broadcast_to(columns[:, t : t + 1], (128, 128))
                        product = column * tiles_ref[first + t]
                        for size in (64, 32, 16):
                            product = product[:size] + product[size:]
                        partial = product.astype(F32)
                        partial = partial[:8] + partial[8:]
                        rows.append(jnp.sum(partial, axis=0, keepdims=True))
                    value = jnp.broadcast_to(rows[3], (8, 128))
                    for j in range(3):
                        value = jnp.where((row8 & 3) == j, rows[j], value)
                    halves.append(value)
            out_ref[pl.ds(base + offset + 8 * h, 8), :] = jnp.where(low, *halves)


def first_kernel(
    count_ref, tiles_ref, rays_ref, rows_ref, slots_ref, wanted_ref,
    *refs,
):
    tiles, turned, refs = refs[:PARTS], refs[PARTS : 2 * PARTS], refs[2 * PARTS :]
    send_ref, rays, st_ref, rt_ref, s_ref, r_ref, g_ref, gt_ref = refs[:8]
    rows, slots, wanted, picked, res, sem, small_sem = refs[8:]
    ntile = tiles_ref.shape[0]
    nrow = rays_ref.shape[0]
    nq = st_ref.shape[0]
    cap, ndev = wanted_ref.shape

    part = ntile // PARTS
    copies = part // CHUNK

    def copy(p, i):
        src = tiles_ref.at[pl.ds(p * part + i * CHUNK, CHUNK)]
        return pltpu.make_async_copy(src, tiles[p].at[pl.ds(i * CHUNK, CHUNK)], sem.at[p, i])

    pairs = ((rows_ref, rows), (rays_ref, rays), (slots_ref, slots), (wanted_ref, wanted))
    small = [pltpu.make_async_copy(a, b, small_sem.at[i]) for i, (a, b) in enumerate(pairs)]
    for c in small:
        c.start()
    for i in range(AHEAD):
        copy(0, i).start()
    for c in small:
        c.wait()
    live = iota((1, ntile), 1) < count_ref[0]
    row_of = jnp.where(live, rows[...], -1)
    slot_of = slots[...]
    slot_of = jnp.where(live, (slot_of >> 1) * ROWS + (slot_of & 1), -1)
    rt = onehot(jnp.broadcast_to(row_of, (nrow, ntile)) == iota((nrow, ntile), 0))
    rt_ref[...] = rt
    r_ref[...] = rt.T
    uraw = rays[...]
    picked[...] = dot(r_ref[...], uraw.astype(BF16)).astype(BF16)
    uu = total(uraw * uraw)
    for i in range(AHEAD, DEPTH):
        copy(0, i).start()
    for p in range(PARTS):
        for i, number in GROUPS[p]:
            for j in range(i // CHUNK, (i + number) // CHUNK):
                copy(p, j).wait()
                n = p * copies + j + DEPTH
                if n < PARTS * copies:
                    copy(n // copies, n % copies).start()
            for j in range(i, i + number):
                turned[p][j] = tiles[p][j].T
            products(picked, tiles[p], res, i, p * part, number)
            if p == 0 and i == 0:
                for q in range(0, nq, 128):
                    st = jnp.broadcast_to(slot_of, (128, ntile)) == iota((128, ntile), 0) + q
                    st = onehot(st)
                    st_ref[q : q + 128, :] = st
                    s_ref[:ntile, q : q + 128] = st.T
                scalar = (iota((EXTRA, nq), 1) & (ROWS - 1) == 2) & (iota((EXTRA, nq), 0) == 0)
                scalar = onehot(scalar)
                s_ref[ntile:, :] = scalar
                req = wanted[...].astype(F32)
                q = iota((nq, ndev), 0)
                peer = q >> 2 == iota((nq, ndev), 1)
                value = jnp.zeros((nq, 128), F32)
                for c in range(cap):
                    column = jnp.broadcast_to(req[c : c + 1, :], (128, ndev)).T.astype(BF16)
                    value = value + dot(onehot(peer & (q & (ROWS - 1) == c)), column)
                value = jnp.where(iota((nq, 128), 0) & (ROWS - 1) < cap, value, -1.0)
                value = value.astype(jnp.int32)
                for b in range(0, BLK_DEV, 128):
                    g = onehot(value == iota((nq, 128), 1) + b)
                    g_ref[:, b : b + 128] = g
                    gt_ref[b : b + 128, :] = g.T
    sums = exact_dot(st_ref[...], res[...])
    send_ref[...] = with_scalar(sums, uu)


def ray_kernel(*refs):
    tiles, turned, refs = refs[:PARTS], refs[PARTS : 2 * PARTS], refs[2 * PARTS :]
    recv_ref, s_ref, st_ref, r_ref, rt_ref, uraw_ref, beta_ref = refs[:7]
    send_ref, uraw_out, alpha_ref, picked, res = refs[7:]
    part = tiles[0].shape[0]
    ntile = PARTS * part

    def run(parts):
        for p in range(PARTS):
            for i in range(0, part, UNROLL):
                products(picked, parts[p], res, i, p * part, UNROLL, VECTOR)

    got = dot(s_ref[...], recv_ref[...])
    picked[...] = got[:ntile].astype(BF16)
    alpha = jnp.sqrt(scalar_total(got[ntile : ntile + 1]))

    run(turned)
    product = exact_dot(rt_ref[...], res[...])
    beta = beta_ref[0:1, 0:1]
    uraw = product / alpha - alpha * (uraw_ref[...] / beta)
    uraw_out[...] = uraw
    alpha_ref[...] = jnp.broadcast_to(alpha, (8, 128))
    picked[...] = dot(r_ref[...], uraw.astype(BF16)).astype(BF16)
    uu = total(uraw * uraw)

    run(tiles)
    sums = exact_dot(st_ref[...], res[...])
    send_ref[...] = with_scalar(sums, uu)


def cell_kernel(first, last, *refs):
    recv_ref, gt_ref = refs[:2]
    recv = recv_ref[...]
    beta = jnp.sqrt(received_total(recv))
    grad = dot(gt_ref[...], recv)
    send_ref, vraw_out, beta_out = refs[-3:]
    vraw = grad / beta
    if not first:
        vraw_ref, alpha_ref = refs[3:5]
        vraw = vraw - beta * (vraw_ref[...] / alpha_ref[0:1, 0:1])
    vraw_out[...] = vraw
    beta_out[...] = jnp.broadcast_to(beta, (8, 128))
    vv = total(vraw * vraw)
    if last:
        send_ref[...] = jnp.broadcast_to(vv, send_ref.shape)
    else:
        send_ref[...] = with_scalar(dot(refs[2][...], vraw.astype(BF16)), vv)


def last_kernel(scale, *refs):
    recv_ref = refs[0]
    vraws = refs[1 : ITERS + 2]
    alphas = [ref[0:1, 0:1] for ref in refs[ITERS + 2 : 2 * ITERS + 2]]
    betas = [ref[0:1, 0:1] for ref in refs[2 * ITERS + 2 : 3 * ITERS + 3]]
    solution_ref, right_ref = refs[3 * ITERS + 3 :]
    vv = jnp.sum(jnp.sum(recv_ref[...], axis=0, keepdims=True)[:, 0:1], axis=1, keepdims=True)
    right_ref[...] = vraws[ITERS][...] * (scale / jnp.sqrt(vv))
    w = vraws[0][...] / alphas[0]
    phibar = betas[0]
    rhobar = alphas[0]
    solution = None
    for step in range(1, ITERS + 1):
        beta = betas[step]
        rhobar1 = jnp.sqrt(rhobar * rhobar + damping * damping)
        phibar = rhobar / rhobar1 * phibar
        rho = jnp.sqrt(rhobar1 * rhobar1 + beta * beta)
        cosine = rhobar1 / rho
        sine = beta / rho
        phi = cosine * phibar
        phibar = sine * phibar
        update = (phi / rho) * w
        solution = update if solution is None else solution + update
        if step < ITERS:
            alpha = alphas[step]
            w = vraws[step][...] / alpha - (sine * alpha / rho) * w
            rhobar = -cosine * alpha
    solution_ref[...] = solution


def shape(dims, dtype=F32):
    return jax.ShapeDtypeStruct(dims, dtype)


VMEM = pl.BlockSpec(memory_space=pltpu.VMEM)
SMEM = pl.BlockSpec(memory_space=pltpu.SMEM)
HBM = pl.BlockSpec(memory_space=pltpu.HBM)


def call(kernel, outs, in_specs, scratch=(), limit=8 << 20):
    if isinstance(in_specs, int):
        in_specs = [VMEM] * in_specs
    return pl.pallas_call(
        kernel,
        out_shape=outs,
        in_specs=in_specs,
        out_specs=[VMEM] * len(outs),
        scratch_shapes=list(scratch),
        compiler_params=pltpu.CompilerParams(vmem_limit_bytes=limit),
    )


def per_device(tiles, rays, tile_rows, tile_slots, tile_count, wanted):
    ndev = lax.axis_size(AXES)
    ntile, _, width = tiles.shape
    nrow = rays.shape[0]
    nq = ndev * ROWS
    cap = wanted.shape[2]

    def exchange(x):
        rows = x.shape[0] // ndev
        y = lax.all_to_all(
            x.reshape(ndev, rows, width), AXES, split_axis=0, concat_axis=0, tiled=True
        )
        return y.reshape(x.shape)

    def far(x):
        return pltpu.with_memory_space_constraint(x, pltpu.HBM)

    cells = shape((BLK_DEV, width))
    scalar = shape((8, width))
    sent = shape((nq, width), BF16)
    scratch = [
        pltpu.VMEM((ntile, width), BF16),
        pltpu.VMEM((ntile, width), F32),
    ]
    *kept, send, uraw, st, rt, s, r, g, gt = call(
        first_kernel,
        [
            *[shape((ntile // PARTS, width, width), BF16)] * (2 * PARTS),
            sent,
            shape((nrow, width)),
            shape((nq, ntile), BF16),
            shape((nrow, ntile), BF16),
            shape((ntile + EXTRA, nq), BF16),
            shape((ntile, nrow), BF16),
            shape((nq, BLK_DEV), BF16),
            shape((BLK_DEV, nq), BF16),
        ],
        [SMEM] + [HBM] * 5,
        [
            pltpu.VMEM((1, ntile), jnp.int32),
            pltpu.VMEM((1, ntile), jnp.int32),
            pltpu.VMEM((cap, ndev), jnp.int32),
            *scratch,
            pltpu.SemaphoreType.DMA((PARTS, ntile // PARTS // CHUNK)),
            pltpu.SemaphoreType.DMA((4,)),
        ],
    )(
        tile_count,
        far(tiles),
        far(rays),
        far(tile_rows.reshape(1, ntile)),
        far(tile_slots.reshape(1, ntile)),
        far(wanted[0].T),
    )

    vraws, alphas, betas = [], [], []
    for step in range(ITERS + 1):
        last = step == ITERS
        if step > 0:
            recv = exchange(send)
            send, uraw, alpha = call(
                ray_kernel,
                [sent, shape((nrow, width)), scalar],
                2 * PARTS + 7,
                scratch,
            )(*kept, recv, s, st, r, rt, uraw, betas[-1])
            alphas.append(alpha)
        recv = exchange(send)
        prior = [] if step == 0 else [vraws[-1], alphas[-1]]
        send, vraw, beta = call(
            functools.partial(cell_kernel, step == 0, last),
            [shape((ndev, width)) if last else sent, cells, scalar],
            3 + len(prior),
        )(recv, gt, g, *prior)
        vraws.append(vraw)
        betas.append(beta)
    recv = exchange(send)
    scale = float(BLK_DEV * width * ndev) ** 0.5
    return tuple(
        call(functools.partial(last_kernel, scale), [cells, cells], 3 * ITERS + 3)(
            recv, *vraws, *alphas, *betas
        )
    )


def solution(mesh):
    split = Mesh(mesh.devices.reshape(4, 4, 4, 2), AXES)
    placed = (
        P(AXES, None, None),
        P(AXES, None),
        P(AXES),
        P(AXES),
        P(AXES),
        P(AXES, None, None),
    )
    return jax.shard_map(
        per_device,
        mesh=split,
        in_specs=placed,
        out_specs=(P(AXES, None), P(AXES, None)),
        check_vma=False,
    )
```
